128 devices in a mesh: owner: 8 (over x, core), rows: 16 (over z, y).
Axes of the slice: x: 4, y: 4, z: 4, core: 2. Of those that a mesh axis runs over, the one named last changes fastest.
Arguments:
- master_gate: float32 [64, 2048, 1024], P('owner', 'rows'), may hold values from -0.1875 to 0.1875
- second_gate: bfloat16 [64, 2048, 1024], P('owner', 'rows'), may hold values from -0.0625 to 0.0625
- master_up: float32 [64, 2048, 1024], P('owner', 'rows'), may hold values from -0.1875 to 0.1875
- second_up: bfloat16 [64, 2048, 1024], P('owner', 'rows'), may hold values from -0.0625 to 0.0625
- master_down: float32 [64, 1024, 2048], P('owner', None, 'rows'), may hold values from -0.25 to 0.25
- second_down: bfloat16 [64, 1024, 2048], P('owner', None, 'rows'), may hold values from -0.09375 to 0.09375
- router_weight: float32 [2048, 64], P('rows', 'owner'), may hold values from -0.125 to 0.125
- router_gain: float32 [2048], P('rows'), may hold values from 0.25 to 1.75
Outputs:
- final_gate: bfloat16 [64, 2048, 1024], P('owner', None, 'rows')
- final_up: bfloat16 [64, 2048, 1024], P('owner', None, 'rows')
- final_down: bfloat16 [64, 1024, 2048], P('owner', 'rows')
- scale_gate: float32 [64, 1024], P('owner', 'rows')
- scale_up: float32 [64, 1024], P('owner', 'rows')
- scale_down: float32 [64, 1024], P('owner', 'rows')
- serve_router: bfloat16 [2048, 64], replicated
The draws below stay inside these ranges and needn't reach their ends.
All inputs are finite; a program needn't handle non-finite values.
Results may differ from the reference program's by a relative error of at most 0.001.
Values may be sent and summed in bfloat16 or wider, within the bound.
No kernel may reach another device: no remote copies, remote signals or barrier semaphores. Data moves between devices by JAX's collectives and lax.ppermute only.
A program may use at most 128 MiB of HBM per device.

```python
import jax
import jax.numpy as jnp
from jax import lax

EXPERTS = 64
D_MODEL = 2048
D_EXPERT = 1024


def with_spikes(values, stream_key, source, target, parts, factor):
    def block_of(position):
        return (jnp.arange(values.shape[position]) // (values.shape[position] // parts)).reshape((-1,) + (1,) * (values.ndim - 1 - position))

    near = jax.random.permutation(stream_key, parts)[block_of(target)]
    second = (block_of(target) + parts // 2) % parts
    return jnp.where((block_of(source) == near) | (block_of(source) == second), factor * values, values)


def shard_levels(rng, extent, shards, low, high):
    level = 1.0
    for axis_at, parts in shards:
        draws = jax.random.uniform(jax.random.fold_in(jax.random.fold_in(rng, 6), axis_at), (parts,), jnp.float32, low / len(shards), high / len(shards))
        level = level * jnp.repeat(jnp.exp(draws), extent[axis_at] // parts).reshape((-1,) + (1,) * (len(extent) - 1 - axis_at))
    return level


def scatter_about(stream_key, dims, scale, bound, shards=(), dtype=jnp.bfloat16):
    entries = jax.random.normal(stream_key, dims, jnp.float32) * scale
    if len(shards) > 0:
        entries = shard_levels(stream_key, dims, shards, -0.22, 0.18) * entries
    return jnp.clip(entries, min=-bound, max=bound).astype(dtype)


def noise_with(key, shape, spread, most, split, heavy, kind=jnp.bfloat16):
    array = spread * jax.random.normal(key, shape, jnp.float32)
    if split:
        array = array * shard_levels(key, shape, split, -0.22, 0.18)
    return jnp.clip(with_spikes(array, jax.random.fold_in(key, 3), *heavy), -most, most).astype(kind)


def setup_inputs(seed: int = 0) -> dict:
    key_of = jax.random.split(jax.random.key(seed), 9)
    return {
        "master_gate": noise_with(key_of[0], (EXPERTS, D_MODEL, D_EXPERT), D_MODEL ** -0.5, 0.1875, ((0, 8), (1, 16)), (1, 2, 16, 2.0), jnp.float32),
        "second_gate": scatter_about(key_of[1], (EXPERTS, D_MODEL, D_EXPERT), (D_MODEL * 4) ** -0.5, 0.0625, ((0, 8), (1, 16))),
        "master_up": noise_with(key_of[2], (EXPERTS, D_MODEL, D_EXPERT), D_MODEL ** -0.5, 0.1875, ((0, 8), (1, 16)), (1, 2, 16, 2.0), jnp.float32),
        "second_up": scatter_about(key_of[3], (EXPERTS, D_MODEL, D_EXPERT), (D_MODEL * 4) ** -0.5, 0.0625, ((0, 8), (1, 16))),
        "master_down": noise_with(key_of[4], (EXPERTS, D_EXPERT, D_MODEL), D_EXPERT ** -0.5, 0.25, ((0, 8), (2, 16)), (2, 1, 16, 2.0), jnp.float32),
        "second_down": scatter_about(key_of[5], (EXPERTS, D_EXPERT, D_MODEL), (D_EXPERT * 4) ** -0.5, 0.09375, ((0, 8), (2, 16))),
        "router_weight": scatter_about(key_of[6], (D_MODEL, EXPERTS), D_MODEL ** -0.5, 0.125, ((0, 16), (1, 8)), jnp.float32),
        "router_gain": jnp.clip(1.0 + 0.15 * jax.random.normal(key_of[7], (D_MODEL,), jnp.float32), 0.25, 1.75),
    }


def reference(master_gate, second_gate, master_up, second_up, master_down, second_down, router_weight, router_gain):
    merged_gate = master_gate + second_gate.astype(jnp.float32)
    merged_up = master_up + second_up.astype(jnp.float32)
    merged_down = master_down + second_down.astype(jnp.float32)
    scale_gate = jnp.sqrt(lax.optimization_barrier(jnp.sum(merged_gate * merged_gate, axis=1)))
    final_gate = (merged_gate / jnp.expand_dims(scale_gate, 1)).astype(jnp.bfloat16)
    scale_up = jnp.sqrt(lax.optimization_barrier(jnp.sum(merged_up * merged_up, axis=1)))
    final_up = (merged_up / jnp.expand_dims(scale_up, 1)).astype(jnp.bfloat16)
    scale_down = jnp.sqrt(lax.optimization_barrier(jnp.sum(merged_down * merged_down, axis=2)))
    final_down = (merged_down / jnp.expand_dims(scale_down, 2)).astype(jnp.bfloat16)
    serve_router = (router_weight * router_gain[:, None]).astype(jnp.bfloat16)
    return (final_gate, final_up, final_down, scale_gate, scale_up, scale_down, serve_router)
```

```python
import jax
import jax.numpy as jnp
from jax import lax
from jax.experimental import pallas as pl
from jax.experimental.pallas import tpu as pltpu
from jax.sharding import PartitionSpec as P

F32, BF16 = jnp.float32, jnp.bfloat16
LANES = 128
MIB = 1 << 20


def cost(flops, moved):
    return pl.CostEstimate(flops=flops, bytes_accessed=moved, transcendentals=0)


def sums_kernel(mg, sg, mu, su, md, sd, w, gain, out, columns):
    e = pl.program_id(0)
    experts = pl.num_programs(0)
    for t, (m, s) in enumerate(((mg, sg), (mu, su))):
        x = m[0] + s[0].astype(F32)
        total = jnp.sum(x * x, axis=0, keepdims=True)
        for g in range(x.shape[1] // LANES):
            out[t * experts + e, g : g + 1, :] = total[:, g * LANES : (g + 1) * LANES]
    x = md[0] + sd[0].astype(F32)
    groups = x.shape[0] // LANES

    @pl.when(e == 0)
    def _():
        columns[...] = jnp.zeros_like(columns)
        piece = (w[...] * gain[...]).astype(BF16).astype(F32)
        out[out.shape[0] - 1] = piece

    lane = lax.broadcasted_iota(jnp.int32, columns.shape, 1)
    held = columns[...]
    for g in range(groups):
        part = x[g * LANES : (g + 1) * LANES]
        total = jnp.sum(part * part, axis=1, keepdims=True)
        held = jnp.where(lane == e * groups + g, total, held)
    columns[...] = held

    @pl.when(e == experts - 1)
    def _():
        rows = columns[...].T
        for k in range(out.shape[0] // 3):
            out[2 * (out.shape[0] // 3) + k] = rows[k * groups : (k + 1) * groups]


def local_sums(mg, sg, mu, su, md, sd, w, gain):
    experts, rows, width = mg.shape
    groups = width // LANES
    tall = pl.BlockSpec((1, rows, width), lambda e: (e, 0, 0))
    flat = pl.BlockSpec((1, width, rows), lambda e: (e, 0, 0))
    whole = lambda a: pl.BlockSpec(a.shape, lambda e: (0,) * a.ndim)
    out = jax.ShapeDtypeStruct((3 * experts + 1, groups, LANES), F32)
    return pl.pallas_call(
        sums_kernel,
        grid=(experts,),
        in_specs=[tall, tall, tall, tall, flat, flat, whole(w), whole(gain)],
        out_specs=whole(out),
        out_shape=out,
        scratch_shapes=[pltpu.VMEM((LANES, LANES), F32)],
        compiler_params=pltpu.CompilerParams(vmem_limit_bytes=16 * MIB),
        cost_estimate=cost(9 * mg.size, 18 * mg.size),
        name="sums",
    )(mg, sg, mu, su, md, sd, w, gain)


def turn_kernel(m, s, out):
    x = m[0] + s[0].astype(F32)
    for g in range(x.shape[1] // LANES):
        out[0, g * LANES : (g + 1) * LANES, :] = x[:, g * LANES : (g + 1) * LANES].T


def turned(m, s, name):
    experts, rows, width = m.shape
    tall = pl.BlockSpec((1, rows, width), lambda e: (e, 0, 0))
    return pl.pallas_call(
        turn_kernel,
        grid=(experts,),
        in_specs=[tall, tall],
        out_specs=pl.BlockSpec((1, width, rows), lambda e: (e, 0, 0)),
        out_shape=jax.ShapeDtypeStruct((experts, width, rows), F32),
        compiler_params=pltpu.CompilerParams(vmem_limit_bytes=8 * MIB),
        cost_estimate=cost(8 * m.size, 10 * m.size),
        name=name,
    )(m, s)


def fold_kernel(sums, a, b, c, d, out):
    out[:sums] = (a[:sums] + b[:sums]) + (c[:sums] + d[:sums])
    pieces = a.shape[0] - sums
    for k, part in enumerate((a, b, c, d)):
        out[sums + k * pieces : sums + (k + 1) * pieces] = part[sums:]


def folded(sums, parts, name):
    pieces = parts[0].shape[0] - sums
    out = jax.ShapeDtypeStruct((sums + 4 * pieces, *parts[0].shape[1:]), F32)
    return pl.pallas_call(
        lambda *refs: fold_kernel(sums, *refs),
        out_shape=out,
        compiler_params=pltpu.CompilerParams(vmem_limit_bytes=4 * MIB),
        cost_estimate=cost(out.size, 24 * out.size),
        name=name,
    )(*parts)


def scale_kernel(a, b, c, d, tg, tu, md, sd, out, scale, kept, inverse):
    e = pl.program_id(0)
    experts = pl.num_programs(0)
    sums = 3 * experts
    groups = tg.shape[1] // LANES

    @pl.when(e == 0)
    def _():
        total = (a[:sums] + b[:sums]) + (c[:sums] + d[:sums])
        root = jnp.sqrt(total)
        scale[...] = root
        pieces = a.shape[0] - sums
        for k, part in enumerate((a, b, c, d)):
            kept[k * pieces : (k + 1) * pieces] = part[sums:]
        flat = (1.0 / root).reshape(sums * groups, LANES)
        pad = jnp.concatenate([flat, flat[: 2 * LANES - sums * groups]], axis=0)
        for k in range(2):
            inverse[:, k * LANES : (k + 1) * LANES] = pad[k * LANES : (k + 1) * LANES].T

    half = LANES // 2
    for t in range(3):
        source = (tg, tu, md)[t]
        at = t * experts * groups + e * groups
        block = inverse[:, (t // 2) * LANES : (t // 2 + 1) * LANES]
        turn = pltpu.roll(block, (2 * LANES - (at - (t // 2) * LANES)) % LANES, 1)
        for g in range(groups):
            rows = slice(g * LANES, (g + 1) * LANES)
            x = source[0, rows, :]
            if t == 2:
                x = x + sd[0, rows, :].astype(F32)
            y = (x * turn[:, g : g + 1]).astype(BF16)
            out[2 * g, t, 0] = y[:half]
            out[2 * g + 1, t, 0] = y[half:]


def scaled(parts, tg, tu, md, sd):
    experts, width, rows = tg.shape
    peers = width // (LANES // 2)
    sums = 3 * experts
    kept = 4 * (parts[0].shape[0] - sums)
    whole = lambda shape: pl.BlockSpec(shape, lambda e: (0,) * len(shape))
    flat = pl.BlockSpec((1, width, rows), lambda e: (e, 0, 0))
    outs = (
        pltpu.HBM((peers, 3, experts, LANES // 2, rows), BF16),
        jax.ShapeDtypeStruct((sums, *parts[0].shape[1:]), F32),
        jax.ShapeDtypeStruct((kept, *parts[0].shape[1:]), F32),
    )
    return pl.pallas_call(
        scale_kernel,
        grid=(experts,),
        in_specs=[whole(p.shape) for p in parts] + [flat] * 4,
        out_specs=(
            pl.BlockSpec((peers, 3, 1, LANES // 2, rows), lambda e: (0, 0, e, 0, 0)),
            whole(outs[1].shape),
            whole(outs[2].shape),
        ),
        out_shape=outs,
        scratch_shapes=[pltpu.VMEM((LANES, 2 * LANES), F32)],
        compiler_params=pltpu.CompilerParams(vmem_limit_bytes=16 * MIB),
        cost_estimate=cost(6 * tg.size, 20 * tg.size),
        name="scaled",
    )(*parts, tg, tu, md, sd)


def gather_kernel(came, g, u, d):
    for t, out in enumerate((g, u, d)):
        for k in range(came.shape[0]):
            out[0, :, k * LANES : (k + 1) * LANES] = came[k, t, 0]


def side_by_side(came):
    peers, _, experts, half, lanes = came.shape
    out = jax.ShapeDtypeStruct((experts, half, peers * lanes), BF16)
    spec = pl.BlockSpec((1, half, peers * lanes), lambda e: (e, 0, 0))
    return pl.pallas_call(
        gather_kernel,
        grid=(experts,),
        in_specs=[pl.BlockSpec((peers, 3, 1, half, lanes), lambda e: (0, 0, e, 0, 0))],
        out_specs=(spec, spec, spec),
        out_shape=(out, out, out),
        compiler_params=pltpu.CompilerParams(vmem_limit_bytes=8 * MIB),
        cost_estimate=cost(0, 4 * came.size),
        name="side_by_side",
    )(came)


def hops(shift_of):
    return [[(i, shift_of(i, k)) for i in range(16)] for k in (1, 2, 3)]


ALONG_Y = hops(lambda i, k: i // 4 * 4 + (i % 4 + k) % 4)
ALONG_Z = hops(lambda i, k: (i // 4 + k) % 4 * 4 + i % 4)
ALONG_X = [[(i, (i // 2 + k) % 4 * 2 + i % 2) for i in range(8)] for k in (1, 2, 3)]
OTHER_CORE = [(i, i ^ 1) for i in range(8)]


def from_all(a, axis, ways):
    return [a] + [lax.ppermute(a, axis, way) for way in ways]


def order_rows_kernel(at, pieces, out):
    z, y = at[0], at[1]
    for a in range(4):
        for b in range(4):
            place = lax.rem(z + 4 - a, 4) * 4 + lax.rem(y + 4 - b, 4)
            out[:, pl.ds(pl.multiple_of(place * LANES, LANES), LANES)] = pieces[4 * a + b].astype(BF16)


def order_owners_kernel(at, mine, other, out):
    x, core = at[2], at[3]
    for k in range(4):
        place = lax.rem(x + 4 - k, 4) * 2
        out[pl.ds(pl.multiple_of((place + core) * 8, 8), 8), :] = mine[k]
        out[pl.ds(pl.multiple_of((place + 1 - core) * 8, 8), 8), :] = other[k]


def placed_by(kernel, at, arrays, shape, name):
    vmem = pl.BlockSpec(memory_space=pltpu.VMEM)
    return pl.pallas_call(
        kernel,
        in_specs=[pl.BlockSpec(memory_space=pltpu.SMEM)] + [vmem] * len(arrays),
        out_specs=vmem,
        out_shape=jax.ShapeDtypeStruct(shape, BF16),
        compiler_params=pltpu.CompilerParams(vmem_limit_bytes=4 * MIB),
        cost_estimate=cost(0, 4 * shape[0] * shape[1]),
        name=name,
    )(at, *arrays)


def in_hbm(a):
    return pltpu.with_memory_space_constraint(a, pltpu.HBM)


def body(mg, sg, mu, su, md, sd, w, gain):
    experts, _, width = mg.shape
    row, own = lax.axis_index("rows"), lax.axis_index("owner")
    z, y = row // 4, row % 4
    sums = 3 * experts
    hbm = [in_hbm(a) for a in (mg, sg, mu, su, md, sd)]
    here = local_sums(*hbm, w.T, gain[None, :])
    near = from_all(here, "rows", ALONG_Y)
    tg = turned(mg, sg, "turn_gate")
    near, tg = lax.optimization_barrier((near, tg))
    line = folded(sums, near, "fold_y")
    far = from_all(line, "rows", ALONG_Z)
    tu = turned(mu, su, "turn_up")
    send, scale, pieces = scaled(far, tg, tu, md, sd)
    came = lax.all_to_all(send, "rows", split_axis=0, concat_axis=0, tiled=True)
    at = jnp.stack([z, y, own // 2, own % 2])
    columns = placed_by(order_rows_kernel, at, (pieces,), (8, 16 * LANES), "order_rows")
    columns = jnp.stack(from_all(columns, "owner", ALONG_X))
    other = lax.ppermute(columns, "owner", OTHER_CORE)
    router = placed_by(order_owners_kernel, at, (columns, other), (64, 16 * LANES), "order_owners").T
    scale = scale.reshape(3, experts, width)
    mine = lax.dynamic_slice_in_dim(scale, row * (width // 16), width // 16, axis=2)
    g, u, d = side_by_side(came)
    return (jnp.swapaxes(g, 1, 2), jnp.swapaxes(u, 1, 2), d, mine[0], mine[1], mine[2], router)


def solution(mesh):
    placed = (
        P("owner", "rows", None),
        P("owner", "rows", None),
        P("owner", "rows", None),
        P("owner", "rows", None),
        P("owner", None, "rows"),
        P("owner", None, "rows"),
        P("rows", "owner"),
        P("rows"),
    )
    return jax.shard_map(
        body,
        mesh=mesh,
        in_specs=placed,
        out_specs=(
            P("owner", None, "rows"),
            P("owner", None, "rows"),
            P("owner", "rows", None),
            P("owner", "rows"),
            P("owner", "rows"),
            P("owner", "rows"),
            P(),
        ),
        check_vma=False,
    )
```

```python
import jax
import jax.numpy as jnp
import numpy as np
from jax import lax
from jax.experimental import pallas as pl
from jax.experimental.pallas import tpu as pltpu
from jax.sharding import PartitionSpec as P

F32, BF16 = jnp.float32, jnp.bfloat16
LANES = 128
MIB = 1 << 20


WAYS = (
    (2, 2), (1, 2), (2, 1), (3, 2), (2, 3), (0, 2), (2, 0),
    (1, 1), (3, 3), (1, 3), (3, 1), (0, 1), (0, 3), (1, 0), (3, 0),
)
ORDER = WAYS + ((0, 0),)
FIRST = 4
GROUPS = ((15, 0, 1, 2, 3, 4, 5, 6), (7, 8, 9, 10), (11, 12, 13, 14))


def away(row, way):
    z, y = lax.div(row, 4) + (way[0] + 4), lax.rem(row, 4) + (way[1] + 4)
    return lax.rem(z, 4) * 4 + lax.rem(y, 4)


def cost(flops, moved):
    return pl.CostEstimate(flops=flops, bytes_accessed=moved, transcendentals=0)


VMEM = pl.BlockSpec(memory_space=pltpu.VMEM)
ANY = pl.BlockSpec(memory_space=pl.ANY)


def sums_kernel(*refs):
    sources, out, held, columns, arrived = refs[:8], refs[8], refs[9:17], refs[17], refs[18]
    experts = sources[0].shape[0]
    groups = sources[4].shape[1] // LANES
    small = [
        pltpu.make_async_copy(sources[i], held[i], arrived.at[6, i - 6]) for i in (6, 7)
    ]
    for copy in small:
        copy.start()

    def fetch(i, e):
        return pltpu.make_async_copy(sources[i].at[e], held[i].at[e], arrived.at[i, e])

    for e in range(experts):
        for i in range(6):
            fetch(i, e).start()
    columns[...] = jnp.zeros_like(columns)
    for copy in small:
        copy.wait()
    out[3 * experts] = (held[6][...] * held[7][...]).astype(BF16).astype(F32)
    lane = lax.broadcasted_iota(jnp.int32, columns.shape, 1)

    def expert(e, carry):
        for i in range(6):
            fetch(i, e).wait()
        for t in range(2):
            m, s = held[2 * t], held[2 * t + 1]
            for g in range(groups):
                part = slice(g * LANES, (g + 1) * LANES)
                x = m[e, :, part] + s[e, :, part].astype(F32)
                out[t * experts + e, g : g + 1, :] = jnp.sum(x * x, axis=0, keepdims=True)
        so_far = columns[...]
        for g in range(groups):
            part = slice(g * LANES, (g + 1) * LANES)
            x = held[4][e, part] + held[5][e, part].astype(F32)
            total = jnp.sum(x * x, axis=1, keepdims=True)
            so_far = jnp.where(lane == e * groups + g, total, so_far)
        columns[...] = so_far
        return carry

    lax.fori_loop(0, experts, expert, 0)
    rows = columns[...].T
    for e in range(experts):
        out[2 * experts + e] = rows[e * groups : (e + 1) * groups]


def local_sums(mg, sg, mu, su, md, sd, w, gain):
    experts, _, width = mg.shape
    arrays = (mg, sg, mu, su, md, sd, w, gain)
    return pl.pallas_call(
        sums_kernel,
        in_specs=[ANY] * 8,
        out_specs=VMEM,
        out_shape=jax.ShapeDtypeStruct((3 * experts + 1, width // LANES, LANES), F32),
        scratch_shapes=[pltpu.VMEM(a.shape, a.dtype) for a in arrays]
        + [pltpu.VMEM((LANES, LANES), F32), pltpu.SemaphoreType.DMA((7, experts))],
        compiler_params=pltpu.CompilerParams(vmem_limit_bytes=24 * MIB),
        cost_estimate=cost(9 * mg.size, 18 * mg.size),
        name="sums",
    )(*arrays)


def turn_kernel(m, s, out):
    x = m[0] + s[0].astype(F32)
    for g in range(x.shape[1] // LANES):
        out[0, g * LANES : (g + 1) * LANES, :] = x[:, g * LANES : (g + 1) * LANES].T


def turned(m, s):
    experts, rows, width = m.shape
    tall = pl.BlockSpec((1, rows, width), lambda e: (e, 0, 0))
    return pl.pallas_call(
        turn_kernel,
        grid=(experts,),
        in_specs=[tall, tall],
        out_specs=pl.BlockSpec((1, width, rows), lambda e: (e, 0, 0)),
        out_shape=jax.ShapeDtypeStruct((experts, width, rows), F32),
        compiler_params=pltpu.CompilerParams(vmem_limit_bytes=8 * MIB),
        cost_estimate=cost(8 * m.size, 10 * m.size),
    )(m, s)


def merge_kernel(m, s, out):
    out[...] = m[...] + s[...].astype(F32)


def merged(m, s):
    flat = pl.BlockSpec((1, *m.shape[1:]), lambda e: (e, 0, 0))
    return pl.pallas_call(
        merge_kernel,
        grid=(m.shape[0],),
        in_specs=[flat, flat],
        out_specs=flat,
        out_shape=jax.ShapeDtypeStruct(m.shape, F32),
        compiler_params=pltpu.CompilerParams(vmem_limit_bytes=8 * MIB),
        cost_estimate=cost(2 * m.size, 10 * m.size),
        name="merge_down",
    )(m, s)


def fold_kernel(sums, a, b, c, d, out):
    out[:sums] = (a[:sums] + b[:sums]) + (c[:sums] + d[:sums])
    pieces = a.shape[0] - sums
    for k, part in enumerate((a, b, c, d)):
        out[sums + k * pieces : sums + (k + 1) * pieces] = part[sums:]


def folded(sums, parts):
    pieces = parts[0].shape[0] - sums
    out = jax.ShapeDtypeStruct((sums + 4 * pieces, *parts[0].shape[1:]), F32)
    return pl.pallas_call(
        lambda *refs: fold_kernel(sums, *refs),
        out_shape=out,
        compiler_params=pltpu.CompilerParams(vmem_limit_bytes=4 * MIB),
        cost_estimate=cost(out.size, 24 * out.size),
    )(*parts)


def in_three(x):
    high = x.astype(BF16).astype(F32)
    middle = (x - high).astype(BF16).astype(F32)
    return [high, middle, (x - high - middle).astype(BF16).astype(F32)]


def picker(combos):
    c = np.arange(LANES)[:, None]
    n = np.arange(combos * LANES)[None, :]
    return jnp.asarray((c % combos == n // LANES) & (c < 3 * combos), BF16)


def divide(first, pick, scales, sources, outs):
    experts, _, lanes = sources[0].shape
    for k, out in enumerate(outs):
        to = away(lax.axis_index("rows"), ORDER[first + k])
        rows = pl.ds(pl.multiple_of(to * out.shape[2], out.shape[2]), out.shape[2])
        for t, source in enumerate(sources):
            combos = slice(t * experts * lanes, (t + 1) * experts * lanes)
            scale = jnp.dot(scales[rows, :], pick[:, combos], preferred_element_type=F32)
            for e in range(experts):
                part = slice(e * lanes, (e + 1) * lanes)
                out[t, e] = (source[e, rows, :] / scale[:, part]).astype(BF16)


def first_kernel(pick, a, b, c, d, tg, tu, td, scale, kept, scales, *outs):
    sums, groups, _ = scale.shape
    root = jnp.sqrt((a[:sums] + b[:sums]) + (c[:sums] + d[:sums]))
    scale[...] = root
    pieces = a.shape[0] - sums
    for k, part in enumerate((a, b, c, d)):
        kept[k * pieces : (k + 1) * pieces] = part[sums:]
    rest = jnp.zeros((LANES - 3 * sums, LANES), F32)
    for g in range(groups):
        block = jnp.concatenate(in_three(root[:, g, :]) + [rest], axis=0)
        scales[g * LANES : (g + 1) * LANES] = block.T.astype(BF16)
    divide(0, pick, scales, (tg, tu, td), outs)


def rest_kernel(first, pick, scales, tg, tu, td, *outs):
    divide(first, pick, scales, (tg, tu, td), outs)


def scaled(pick, parts, tg, tu, td, ends):
    experts, width, rows = tg.shape
    peers = len(ORDER)
    sums = 3 * experts
    piece = pltpu.VMEM((3, experts, width // peers, rows), BF16)
    size = 3 * experts * (width // peers) * rows
    outs = [
        jax.ShapeDtypeStruct((sums, *parts[0].shape[1:]), F32),
        jax.ShapeDtypeStruct((4 * (parts[0].shape[0] - sums), *parts[0].shape[1:]), F32),
        pltpu.VMEM((width, LANES), BF16),
    ]
    moved = lambda count: 6 * count * size
    scale, kept, scales, *pieces = pl.pallas_call(
        first_kernel,
        in_specs=[VMEM] * 8,
        out_specs=[VMEM] * (3 + ends[0]),
        out_shape=outs + [piece] * ends[0],
        compiler_params=pltpu.CompilerParams(vmem_limit_bytes=8 * MIB),
        cost_estimate=cost(6 * size * ends[0], moved(ends[0])),
        name="scale_0",
    )(pick, *parts, tg, tu, td)
    for first, end in zip(ends, ends[1:]):
        pieces += pl.pallas_call(
            lambda *refs, first=first: rest_kernel(first, *refs),
            in_specs=[VMEM] * 5,
            out_specs=[VMEM] * (end - first),
            out_shape=[piece] * (end - first),
            compiler_params=pltpu.CompilerParams(vmem_limit_bytes=8 * MIB),
            cost_estimate=cost(6 * size * (end - first), moved(end - first)),
        )(pick, scales, tg, tu, td)
    return scale, kept, pieces


def place_kernel(ways, *refs):
    count = len(ways)
    pieces, outs, done = refs[:count], refs[-4:-1], refs[-1]
    copies = []
    for k, piece in enumerate(pieces):
        back = [-step for step in ways[k]]
        came_from = away(lax.axis_index("rows"), back)
        columns = pl.ds(pl.multiple_of(came_from * LANES, LANES), LANES)
        for t, out in enumerate(outs):
            copies.append(pltpu.make_async_copy(piece.at[t], out.at[:, :, columns], done.at[k, t]))
    for copy in copies:
        copy.start()
    for copy in copies:
        copy.wait()


def side_by_side(pieces, groups):
    _, experts, rows, lanes = pieces[0].shape
    out = pltpu.HBM((experts, rows, len(ORDER) * lanes), BF16)
    so_far = ()
    for group in groups:
        count = len(group)
        ways = [ORDER[k] for k in group]
        so_far = pl.pallas_call(
            lambda *refs, ways=ways: place_kernel(ways, *refs),
            in_specs=[VMEM] * count + [ANY] * len(so_far),
            out_specs=[ANY] * 3,
            out_shape=[out] * 3,
            scratch_shapes=[pltpu.SemaphoreType.DMA((count, 3))],
            input_output_aliases={count + t: t for t in range(len(so_far))},
            compiler_params=pltpu.CompilerParams(vmem_limit_bytes=8 * MIB),
            cost_estimate=cost(0, 4 * count * pieces[0].size),
        )(*[pieces[k] for k in group], *so_far)
    return so_far


def order_rows_kernel(pieces, out):
    for a in range(4):
        for b in range(4):
            place = away(lax.axis_index("rows"), (-a, -b))
            out[:, pl.ds(pl.multiple_of(place * LANES, LANES), LANES)] = pieces[4 * a + b].astype(BF16)


def stack_kernel(a, b, c, d, out):
    for k, part in enumerate((a, b, c, d)):
        out[k] = part[...]


def own_scales_kernel(scale, *outs):
    row = lax.axis_index("rows")
    experts, width = outs[0].shape
    group, half = lax.div(row * width, LANES), lax.rem(row * width, LANES)
    for t, out in enumerate(outs):
        x = scale[t * experts : (t + 1) * experts, group, :]
        out[...] = jnp.where(half > 0, pltpu.roll(x, LANES - width, 1), x)[:, :width]


def own_scales(scale, experts):
    out = jax.ShapeDtypeStruct((experts, 64), F32)
    return pl.pallas_call(
        own_scales_kernel,
        in_specs=[VMEM],
        out_specs=[VMEM] * 3,
        out_shape=[out] * 3,
        compiler_params=pltpu.CompilerParams(vmem_limit_bytes=4 * MIB),
        cost_estimate=cost(0, 4 * scale.size),
        name="own_scales",
    )(scale)


def order_owners_kernel(a, b, c, d, other, out):
    own = lax.axis_index("owner")
    x, core = lax.div(own, 2), lax.rem(own, 2)
    for k in range(4):
        place = lax.rem(x + 4 - k, 4) * 2
        out[pl.ds(pl.multiple_of((place + core) * 8, 8), 8), :] = (a, b, c, d)[k][...]
        out[pl.ds(pl.multiple_of((place + 1 - core) * 8, 8), 8), :] = other[k]


def placed_by(kernel, arrays, shape):
    return pl.pallas_call(
        kernel,
        in_specs=[VMEM] * len(arrays),
        out_specs=VMEM,
        out_shape=jax.ShapeDtypeStruct(shape, BF16),
        compiler_params=pltpu.CompilerParams(vmem_limit_bytes=4 * MIB),
        cost_estimate=cost(0, 1 << 18),
    )(*arrays)


def in_hbm(a):
    return pltpu.with_memory_space_constraint(a, pltpu.HBM)


def pairs(way):
    return [(i, (i // 4 + way[0]) % 4 * 4 + (i % 4 + way[1]) % 4) for i in range(16)]


ALONG_Y = [pairs((0, k)) for k in (1, 2, 3)]
ALONG_Z = [pairs((k, 0)) for k in (1, 2, 3)]
ALONG_X = [[(i, (i // 2 + k) % 4 * 2 + i % 2) for i in range(8)] for k in (1, 2, 3)]
OTHER_CORE = [(i, i ^ 1) for i in range(8)]


def from_all(a, axis, ways):
    came = [a]
    for way in ways:
        came.append(lax.ppermute(a, axis, way))
    return came


def body(mg, sg, mu, su, md, sd, w, gain):
    experts = mg.shape[0]
    sums = 3 * experts
    here = local_sums(*[in_hbm(a) for a in (mg, sg, mu, su, md, sd, w.T, gain[None, :])])
    near = from_all(here, "rows", ALONG_Y)
    line = folded(sums, near)
    far = from_all(line, "rows", ALONG_Z)
    tg = turned(mg, sg)
    tu = turned(mu, su)
    td = merged(md, sd)
    scale, pieces, send = scaled(picker(sums), far, tg, tu, td, (FIRST, 16))
    came = []
    for k, way in enumerate(WAYS):
        came.append(lax.ppermute(send[k], "rows", pairs(way)))
    came.append(send[-1])
    columns = placed_by(order_rows_kernel, (pieces,), (8, 16 * LANES))
    columns = from_all(columns, "owner", ALONG_X)
    other = lax.ppermute(placed_by(stack_kernel, columns, (4, 8, 16 * LANES)), "owner", OTHER_CORE)
    router = placed_by(order_owners_kernel, (*columns, other), (64, 16 * LANES)).T
    mine = own_scales(scale, experts)
    g, u, d = side_by_side(came, GROUPS)
    return (jnp.swapaxes(g, 1, 2), jnp.swapaxes(u, 1, 2), d, mine[0], mine[1], mine[2], router)


def solution(mesh):
    placed = (
        P("owner", "rows", None),
        P("owner", "rows", None),
        P("owner", "rows", None),
        P("owner", "rows", None),
        P("owner", None, "rows"),
        P("owner", None, "rows"),
        P("rows", "owner"),
        P("rows"),
    )
    return jax.shard_map(
        body,
        mesh=mesh,
        in_specs=placed,
        out_specs=(
            P("owner", None, "rows"),
            P("owner", None, "rows"),
            P("owner", "rows", None),
            P("owner", "rows"),
            P("owner", "rows"),
            P("owner", "rows"),
            P(),
        ),
        check_vma=False,
    )
```

```python
import jax
import jax.numpy as jnp
import numpy as np
from jax import lax
from jax.experimental import pallas as pl
from jax.experimental.pallas import tpu as pltpu
from jax.sharding import PartitionSpec as P

F32, BF16 = jnp.float32, jnp.bfloat16
LANES = 128
MIB = 1 << 20


SETS = 4
STEPS = (2, 1, 3)
GROUPS = (
    tuple((k, i) for k in (0, 1) for i in range(4)),
    tuple((k, i) for k in (2, 3) for i in (0, 1, 3)),
    tuple((k, 2) for k in (2, 3)),
)


def away(row, way):
    z, y = lax.div(row, 4) + (way[0] + 4), lax.rem(row, 4) + (way[1] + 4)
    return lax.rem(z, 4) * 4 + lax.rem(y, 4)


def cost(flops, moved):
    return pl.CostEstimate(flops=flops, bytes_accessed=moved, transcendentals=0)


VMEM = pl.BlockSpec(memory_space=pltpu.VMEM)
ANY = pl.BlockSpec(memory_space=pl.ANY)


def sums_kernel(*refs):
    sources, out, held, columns, arrived = refs[:8], refs[8], refs[9:17], refs[17], refs[18]
    experts = sources[0].shape[0]
    groups = sources[4].shape[1] // LANES
    small = [
        pltpu.make_async_copy(sources[i], held[i], arrived.at[6, i - 6]) for i in (6, 7)
    ]
    for copy in small:
        copy.start()

    def fetch(i, e):
        return pltpu.make_async_copy(sources[i].at[e], held[i].at[e], arrived.at[i, e])

    for e in range(experts):
        for i in range(6):
            fetch(i, e).start()
    columns[...] = jnp.zeros_like(columns)
    for copy in small:
        copy.wait()
    out[3 * experts] = (held[6][...] * held[7][...]).astype(BF16).astype(F32)
    lane = lax.broadcasted_iota(jnp.int32, columns.shape, 1)

    def expert(e, carry):
        for i in range(6):
            fetch(i, e).wait()
        for t in range(2):
            m, s = held[2 * t], held[2 * t + 1]
            for g in range(groups):
                part = slice(g * LANES, (g + 1) * LANES)
                x = m[e, :, part] + s[e, :, part].astype(F32)
                out[t * experts + e, g : g + 1, :] = jnp.sum(x * x, axis=0, keepdims=True)
        so_far = columns[...]
        for g in range(groups):
            part = slice(g * LANES, (g + 1) * LANES)
            x = held[4][e, part] + held[5][e, part].astype(F32)
            total = jnp.sum(x * x, axis=1, keepdims=True)
            so_far = jnp.where(lane == e * groups + g, total, so_far)
        columns[...] = so_far
        return carry

    lax.fori_loop(0, experts, expert, 0)
    rows = columns[...].T
    for e in range(experts):
        out[2 * experts + e] = rows[e * groups : (e + 1) * groups]


def local_sums(mg, sg, mu, su, md, sd, w, gain):
    experts, _, width = mg.shape
    arrays = (mg, sg, mu, su, md, sd, w, gain)
    return pl.pallas_call(
        sums_kernel,
        in_specs=[ANY] * 8,
        out_specs=VMEM,
        out_shape=jax.ShapeDtypeStruct((3 * experts + 1, width // LANES, LANES), F32),
        scratch_shapes=[pltpu.VMEM(a.shape, a.dtype) for a in arrays]
        + [pltpu.VMEM((LANES, LANES), F32), pltpu.SemaphoreType.DMA((7, experts))],
        compiler_params=pltpu.CompilerParams(vmem_limit_bytes=24 * MIB),
        cost_estimate=cost(9 * mg.size, 18 * mg.size),
        name="sums",
    )(*arrays)


def turn_kernel(m, s, out):
    x = m[0] + s[0].astype(F32)
    for g in range(x.shape[1] // LANES):
        out[0, g * LANES : (g + 1) * LANES, :] = x[:, g * LANES : (g + 1) * LANES].T


def turned(m, s):
    experts, rows, width = m.shape
    tall = pl.BlockSpec((1, rows, width), lambda e: (e, 0, 0))
    return pl.pallas_call(
        turn_kernel,
        grid=(experts,),
        in_specs=[tall, tall],
        out_specs=pl.BlockSpec((1, width, rows), lambda e: (e, 0, 0)),
        out_shape=jax.ShapeDtypeStruct((experts, width, rows), F32),
        compiler_params=pltpu.CompilerParams(vmem_limit_bytes=8 * MIB),
        cost_estimate=cost(8 * m.size, 10 * m.size),
    )(m, s)


def merge_kernel(m, s, out):
    out[...] = m[...] + s[...].astype(F32)


def merged(m, s):
    flat = pl.BlockSpec((1, *m.shape[1:]), lambda e: (e, 0, 0))
    return pl.pallas_call(
        merge_kernel,
        grid=(m.shape[0],),
        in_specs=[flat, flat],
        out_specs=flat,
        out_shape=jax.ShapeDtypeStruct(m.shape, F32),
        compiler_params=pltpu.CompilerParams(vmem_limit_bytes=8 * MIB),
        cost_estimate=cost(2 * m.size, 10 * m.size),
        name="merge_down",
    )(m, s)


def fold_kernel(sums, a, b, c, d, out):
    out[:sums] = (a[:sums] + b[:sums]) + (c[:sums] + d[:sums])
    pieces = a.shape[0] - sums
    for k, part in enumerate((a, b, c, d)):
        out[sums + k * pieces : sums + (k + 1) * pieces] = part[sums:]


def folded(sums, parts):
    pieces = parts[0].shape[0] - sums
    out = jax.ShapeDtypeStruct((sums + 4 * pieces, *parts[0].shape[1:]), F32)
    return pl.pallas_call(
        lambda *refs: fold_kernel(sums, *refs),
        out_shape=out,
        compiler_params=pltpu.CompilerParams(vmem_limit_bytes=4 * MIB),
        cost_estimate=cost(out.size, 24 * out.size),
    )(*parts)


def in_three(x):
    high = x.astype(BF16).astype(F32)
    middle = (x - high).astype(BF16).astype(F32)
    return [high, middle, (x - high - middle).astype(BF16).astype(F32)]


def picker(combos):
    c = np.arange(LANES)[:, None]
    n = np.arange(combos * LANES)[None, :]
    return jnp.asarray((c % combos == n // LANES) & (c < 3 * combos), BF16)


def divide(which, pick, scales, sources, outs):
    experts, _, lanes = sources[0].shape
    _, _, share, width, _ = outs[0].shape
    for step, out in zip((0,) + STEPS, outs):
        for i in range(4):
            way = (i, step) if which % 2 == 0 else (step, i)
            to = away(lax.axis_index("rows"), way)
            rows = pl.ds(pl.multiple_of(to * width, width), width)
            for t, source in enumerate(sources):
                first = (t * experts + which * share) * lanes
                combos = slice(first, first + share * lanes)
                scale = jnp.dot(scales[rows, :], pick[:, combos], preferred_element_type=F32)
                for e in range(share):
                    part = slice(e * lanes, (e + 1) * lanes)
                    x = source[which * share + e, rows, :]
                    out[i, t, e] = (x / scale[:, part]).astype(BF16)


def first_kernel(sets, pick, a, b, c, d, tg, tu, td, scale, kept, scales, *outs):
    sums, groups, _ = scale.shape
    root = jnp.sqrt((a[:sums] + b[:sums]) + (c[:sums] + d[:sums]))
    scale[...] = root
    pieces = a.shape[0] - sums
    for k, part in enumerate((a, b, c, d)):
        kept[k * pieces : (k + 1) * pieces] = part[sums:]
    rest = jnp.zeros((LANES - 3 * sums, LANES), F32)
    for g in range(groups):
        block = jnp.concatenate(in_three(root[:, g, :]) + [rest], axis=0)
        scales[g * LANES : (g + 1) * LANES] = block.T.astype(BF16)
    for k, which in enumerate(sets):
        divide(which, pick, scales, (tg, tu, td), outs[4 * k : 4 * k + 4])


def rest_kernel(sets, pick, scales, tg, tu, td, *outs):
    for k, which in enumerate(sets):
        divide(which, pick, scales, (tg, tu, td), outs[4 * k : 4 * k + 4])


def scaled(pick, parts, tg, tu, td):
    experts, width, rows = tg.shape
    sums = 3 * experts
    piece = pltpu.VMEM((4, 3, experts // SETS, width // 16, rows), BF16)
    outs = [
        jax.ShapeDtypeStruct((sums, *parts[0].shape[1:]), F32),
        jax.ShapeDtypeStruct((4 * (parts[0].shape[0] - sums), *parts[0].shape[1:]), F32),
        pltpu.VMEM((width, LANES), BF16),
    ]
    spent = cost(3 * tg.size, 9 * tg.size)
    params = pltpu.CompilerParams(vmem_limit_bytes=8 * MIB)
    scale, kept, scales, *pieces = pl.pallas_call(
        lambda *refs: first_kernel((0, 1), *refs),
        in_specs=[VMEM] * 8,
        out_specs=[VMEM] * 11,
        out_shape=outs + [piece] * 8,
        compiler_params=params,
        cost_estimate=spent,
        name="scale_0",
    )(pick, *parts, tg, tu, td)
    pieces += pl.pallas_call(
        lambda *refs: rest_kernel((2, 3), *refs),
        in_specs=[VMEM] * 5,
        out_specs=[VMEM] * 8,
        out_shape=[piece] * 8,
        compiler_params=params,
        cost_estimate=spent,
        name="scale_2",
    )(pick, scales, tg, tu, td)
    return scale, kept, [pieces[4 * k : 4 * k + 4] for k in range(SETS)]


def turn_corner_kernel(*refs):
    came, outs = refs[:4], refs[4:]
    for i, out in enumerate(outs):
        for j in range(4):
            out[j] = came[j][i]


def turn_corner(came):
    out = pltpu.VMEM(came[0].shape, BF16)
    return pl.pallas_call(
        turn_corner_kernel,
        in_specs=[VMEM] * 4,
        out_specs=[VMEM] * 4,
        out_shape=[out] * 4,
        compiler_params=pltpu.CompilerParams(vmem_limit_bytes=4 * MIB),
        cost_estimate=cost(0, 16 * came[0].size),
    )(*came)


def place_kernel(picks, *refs):
    outs, done = refs[-4:-1], refs[-1]
    copies = []
    for n, ((which, i), came) in enumerate(zip(picks, refs)):
        _, _, share, _, lanes = came.shape
        for j, step in enumerate((0,) + STEPS):
            back = (-i, -step) if which % 2 == 0 else (-step, -i)
            sender = away(lax.axis_index("rows"), back)
            columns = pl.ds(pl.multiple_of(sender * lanes, lanes), lanes)
            for t, out in enumerate(outs):
                to = out.at[which * share : (which + 1) * share, :, columns]
                copies.append(pltpu.make_async_copy(came.at[j, t], to, done.at[4 * n + j, t]))
    for copy in copies:
        copy.start()
    for copy in copies:
        copy.wait()


def side_by_side(sets, groups):
    _, _, share, rows, lanes = sets[0][0].shape
    out = pltpu.HBM((SETS * share, rows, 16 * lanes), BF16)
    so_far = ()
    for picks in groups:
        n = len(picks)
        so_far = pl.pallas_call(
            lambda *refs, picks=picks: place_kernel(picks, *refs),
            in_specs=[VMEM] * n + [ANY] * len(so_far),
            out_specs=[ANY] * 3,
            out_shape=[out] * 3,
            scratch_shapes=[pltpu.SemaphoreType.DMA((4 * n, 3))],
            input_output_aliases={n + t: t for t in range(len(so_far))},
            compiler_params=pltpu.CompilerParams(vmem_limit_bytes=8 * MIB),
            cost_estimate=cost(0, 4 * n * sets[0][0].size),
        )(*[sets[which][i] for which, i in picks], *so_far)
    return so_far


def order_rows_kernel(pieces, out):
    for a in range(4):
        for b in range(4):
            place = away(lax.axis_index("rows"), (-a, -b))
            out[:, pl.ds(pl.multiple_of(place * LANES, LANES), LANES)] = pieces[4 * a + b].astype(BF16)


def stack_kernel(a, b, c, d, out):
    for k, part in enumerate((a, b, c, d)):
        out[k] = part[...]


def own_scales_kernel(scale, *outs):
    row = lax.axis_index("rows")
    experts, width = outs[0].shape
    group, half = lax.div(row * width, LANES), lax.rem(row * width, LANES)
    for t, out in enumerate(outs):
        x = scale[t * experts : (t + 1) * experts, group, :]
        out[...] = jnp.where(half > 0, pltpu.roll(x, LANES - width, 1), x)[:, :width]


def own_scales(scale, experts):
    out = jax.ShapeDtypeStruct((experts, 64), F32)
    return pl.pallas_call(
        own_scales_kernel,
        in_specs=[VMEM],
        out_specs=[VMEM] * 3,
        out_shape=[out] * 3,
        compiler_params=pltpu.CompilerParams(vmem_limit_bytes=4 * MIB),
        cost_estimate=cost(0, 4 * scale.size),
        name="own_scales",
    )(scale)


def order_owners_kernel(a, b, c, d, other, out):
    own = lax.axis_index("owner")
    x, core = lax.div(own, 2), lax.rem(own, 2)
    for k in range(4):
        place = lax.rem(x + 4 - k, 4) * 2
        out[pl.ds(pl.multiple_of((place + core) * 8, 8), 8), :] = (a, b, c, d)[k][...]
        out[pl.ds(pl.multiple_of((place + 1 - core) * 8, 8), 8), :] = other[k]


def placed_by(kernel, arrays, shape):
    return pl.pallas_call(
        kernel,
        in_specs=[VMEM] * len(arrays),
        out_specs=VMEM,
        out_shape=jax.ShapeDtypeStruct(shape, BF16),
        compiler_params=pltpu.CompilerParams(vmem_limit_bytes=4 * MIB),
        cost_estimate=cost(0, 1 << 18),
    )(*arrays)


def in_hbm(a):
    return pltpu.with_memory_space_constraint(a, pltpu.HBM)


def pairs(way):
    return [(i, (i // 4 + way[0]) % 4 * 4 + (i % 4 + way[1]) % 4) for i in range(16)]


ALONG_Y = [pairs((0, k)) for k in (1, 2, 3)]
ALONG_Z = [pairs((k, 0)) for k in (1, 2, 3)]
ALONG_X = [[(i, (i // 2 + k) % 4 * 2 + i % 2) for i in range(8)] for k in (1, 2, 3)]
OTHER_CORE = [(i, i ^ 1) for i in range(8)]


def from_all(a, axis, ways):
    came = [a]
    for way in ways:
        came.append(lax.ppermute(a, axis, way))
    return came


def body(mg, sg, mu, su, md, sd, w, gain):
    experts = mg.shape[0]
    sums = 3 * experts
    here = local_sums(*[in_hbm(a) for a in (mg, sg, mu, su, md, sd, w.T, gain[None, :])])
    near = from_all(here, "rows", ALONG_Y)
    line = folded(sums, near)
    far = from_all(line, "rows", ALONG_Z)
    tg = turned(mg, sg)
    tu = turned(mu, su)
    td = merged(md, sd)
    scale, pieces, send = scaled(picker(sums), far, tg, tu, td)
    ways = {k: (pairs((0, k)), pairs((k, 0))) for k in STEPS}
    half = [[parts[0]] for parts in send]
    for k, step in sent_in_order():
        part = send[k][1 + STEPS.index(step)]
        half[k].append(lax.ppermute(part, "rows", ways[step][k % 2]))
    came = []
    for k in range(SETS):
        parts = turn_corner(half[k])
        whole = [parts[0]] * 4
        for step in STEPS:
            whole[step] = lax.ppermute(parts[step], "rows", ways[step][1 - k % 2])
        came.append(whole)
    columns = placed_by(order_rows_kernel, (pieces,), (8, 16 * LANES))
    columns = from_all(columns, "owner", ALONG_X)
    other = lax.ppermute(placed_by(stack_kernel, columns, (4, 8, 16 * LANES)), "owner", OTHER_CORE)
    router = placed_by(order_owners_kernel, (*columns, other), (64, 16 * LANES)).T
    mine = own_scales(scale, experts)
    g, u, d = side_by_side(came, GROUPS)
    return (jnp.swapaxes(g, 1, 2), jnp.swapaxes(u, 1, 2), d, mine[0], mine[1], mine[2], router)


def sent_in_order(steps=STEPS):
    return [(k + i, step) for k in range(0, SETS, 2) for step in steps for i in (0, 1)]


def solution(mesh):
    placed = (
        P("owner", "rows", None),
        P("owner", "rows", None),
        P("owner", "rows", None),
        P("owner", "rows", None),
        P("owner", None, "rows"),
        P("owner", None, "rows"),
        P("rows", "owner"),
        P("rows"),
    )
    return jax.shard_map(
        body,
        mesh=mesh,
        in_specs=placed,
        out_specs=(
            P("owner", None, "rows"),
            P("owner", None, "rows"),
            P("owner", "rows", None),
            P("owner", "rows"),
            P("owner", "rows"),
            P("owner", "rows"),
            P(),
        ),
        check_vma=False,
    )
```

```python
import jax
import jax.numpy as jnp
import numpy as np
from jax import lax
from jax.experimental import pallas as pl
from jax.experimental.pallas import tpu as pltpu
from jax.sharding import PartitionSpec as P

F32, BF16 = jnp.float32, jnp.bfloat16
LANES = 128
MIB = 1 << 20


SHARES = (3, 3, 1, 1)
STARTS = (0, 3, 6, 7)
SETS = len(SHARES)
STEPS = (2, 1, 3)
NEAR = (0, 2, 1, 3)
GROUPS = (
    tuple((k, 0) for k in range(SETS)),
    ((0, 1), (1, 1), (0, 3), (1, 3)),
    ((0, 2), (1, 2), (2, 1), (3, 1), (2, 3), (3, 3)),
    ((2, 2), (3, 2)),
)


def away(row, way):
    z, y = lax.div(row, 4) + (way[0] + 4), lax.rem(row, 4) + (way[1] + 4)
    return lax.rem(z, 4) * 4 + lax.rem(y, 4)


def cost(flops, moved):
    return pl.CostEstimate(flops=flops, bytes_accessed=moved, transcendentals=0)


VMEM = pl.BlockSpec(memory_space=pltpu.VMEM)
ANY = pl.BlockSpec(memory_space=pl.ANY)


def sums_kernel(*refs):
    sources, out, merged, held = refs[:8], refs[8], refs[9:12], refs[12:20]
    columns, arrived = refs[20], refs[21]
    experts = sources[0].shape[0]
    groups = sources[4].shape[1] // LANES
    small = [
        pltpu.make_async_copy(sources[i], held[i], arrived.at[6, i - 6]) for i in (6, 7)
    ]
    for copy in small:
        copy.start()

    def fetch(i, e):
        return pltpu.make_async_copy(sources[i].at[e], held[i].at[e], arrived.at[i, e])

    for e in range(experts):
        for i in range(6):
            fetch(i, e).start()
    columns[...] = jnp.zeros_like(columns)
    for copy in small:
        copy.wait()
    out[3 * experts] = (held[6][...] * held[7][...]).astype(BF16).astype(F32)
    lane = lax.broadcasted_iota(jnp.int32, columns.shape, 1)

    def expert(e, carry):
        for i in range(6):
            fetch(i, e).wait()
        for t in range(2):
            m, s = held[2 * t], held[2 * t + 1]
            for g in range(groups):
                part = slice(g * LANES, (g + 1) * LANES)
                x = m[e, :, part] + s[e, :, part].astype(F32)
                merged[t][e, :, part] = x
                out[t * experts + e, g : g + 1, :] = jnp.sum(x * x, axis=0, keepdims=True)
        so_far = columns[...]
        for g in range(groups):
            part = slice(g * LANES, (g + 1) * LANES)
            x = held[4][e, part] + held[5][e, part].astype(F32)
            merged[2][e, part] = x
            total = jnp.sum(x * x, axis=1, keepdims=True)
            so_far = jnp.where(lane == e * groups + g, total, so_far)
        columns[...] = so_far
        return carry

    lax.fori_loop(0, experts, expert, 0)
    rows = columns[...].T
    for e in range(experts):
        out[2 * experts + e] = rows[e * groups : (e + 1) * groups]


def local_sums(mg, sg, mu, su, md, sd, w, gain):
    experts, _, width = mg.shape
    arrays = (mg, sg, mu, su, md, sd, w, gain)
    return pl.pallas_call(
        sums_kernel,
        in_specs=[ANY] * 8,
        out_specs=[VMEM] * 4,
        out_shape=[jax.ShapeDtypeStruct((3 * experts + 1, width // LANES, LANES), F32)]
        + [pltpu.VMEM(a.shape, F32) for a in (mg, mu, md)],
        scratch_shapes=[pltpu.VMEM(a.shape, a.dtype) for a in arrays]
        + [pltpu.VMEM((LANES, LANES), F32), pltpu.SemaphoreType.DMA((7, experts))],
        compiler_params=pltpu.CompilerParams(vmem_limit_bytes=20 * MIB),
        cost_estimate=cost(9 * mg.size, 18 * mg.size),
        name="sums",
    )(*arrays)


def turn_kernel(m, out):
    for g in range(m.shape[2] // LANES):
        out[0, g * LANES : (g + 1) * LANES, :] = m[0, :, g * LANES : (g + 1) * LANES].T


def turned(m):
    experts, rows, width = m.shape
    return pl.pallas_call(
        turn_kernel,
        grid=(experts,),
        in_specs=[pl.BlockSpec((1, rows, width), lambda e: (e, 0, 0))],
        out_specs=pl.BlockSpec((1, width, rows), lambda e: (e, 0, 0)),
        out_shape=jax.ShapeDtypeStruct((experts, width, rows), F32),
        compiler_params=pltpu.CompilerParams(vmem_limit_bytes=8 * MIB),
        cost_estimate=cost(8 * m.size, 8 * m.size),
    )(m)


def fold_kernel(sums, a, b, c, d, out):
    out[:sums] = (a[:sums] + b[:sums]) + (c[:sums] + d[:sums])
    pieces = a.shape[0] - sums
    for k, part in enumerate((a, b, c, d)):
        out[sums + k * pieces : sums + (k + 1) * pieces] = part[sums:]


def folded(sums, parts):
    pieces = parts[0].shape[0] - sums
    out = jax.ShapeDtypeStruct((sums + 4 * pieces, *parts[0].shape[1:]), F32)
    return pl.pallas_call(
        lambda *refs: fold_kernel(sums, *refs),
        out_shape=out,
        compiler_params=pltpu.CompilerParams(vmem_limit_bytes=4 * MIB),
        cost_estimate=cost(out.size, 24 * out.size),
    )(*parts)


def in_three(x):
    high = x.astype(BF16).astype(F32)
    middle = (x - high).astype(BF16).astype(F32)
    return [high, middle, (x - high - middle).astype(BF16).astype(F32)]


def picker(combos):
    c = np.arange(LANES)[:, None]
    n = np.arange(combos * LANES)[None, :]
    return jnp.asarray((c % combos == n // LANES) & (c < 3 * combos), BF16)


def divide(picks, pick, scales, sources, outs):
    experts, _, lanes = sources[0].shape
    for (which, step), out in zip(picks, outs):
        _, _, share, width, _ = out.shape
        for i in range(4):
            way = (i, step) if which % 2 == 0 else (step, i)
            to = away(lax.axis_index("rows"), way)
            rows = pl.ds(pl.multiple_of(to * width, width), width)
            for t, source in enumerate(sources):
                first = (t * experts + STARTS[which]) * lanes
                combos = slice(first, first + share * lanes)
                scale = jnp.dot(scales[rows, :], pick[:, combos], preferred_element_type=F32)
                for e in range(share):
                    part = slice(e * lanes, (e + 1) * lanes)
                    x = source[STARTS[which] + e, rows, :]
                    out[i, t, e] = (x / scale[:, part]).astype(BF16)


def first_kernel(picks, pick, a, b, c, d, tg, tu, td, scale, kept, scales, *outs):
    sums, groups, _ = scale.shape
    root = jnp.sqrt((a[:sums] + b[:sums]) + (c[:sums] + d[:sums]))
    scale[...] = root
    pieces = a.shape[0] - sums
    for k, part in enumerate((a, b, c, d)):
        kept[k * pieces : (k + 1) * pieces] = part[sums:]
    rest = jnp.zeros((LANES - 3 * sums, LANES), F32)
    for g in range(groups):
        block = jnp.concatenate(in_three(root[:, g, :]) + [rest], axis=0)
        scales[g * LANES : (g + 1) * LANES] = block.T.astype(BF16)
    divide(picks, pick, scales, (tg, tu, td), outs)


def rest_kernel(picks, pick, scales, tg, tu, td, *outs):
    divide(picks, pick, scales, (tg, tu, td), outs)


def scaled(pick, parts, tg, tu, td):
    experts, width, rows = tg.shape
    sums = 3 * experts
    made = lambda k: pltpu.VMEM((4, 3, SHARES[k], width // 16, rows), BF16)
    early = [(k, STEPS[0]) for k in (0, 1)]
    late = [(k, step) for k in range(SETS) for step in STEPS + (0,) if (k, step) not in early]
    outs = [
        jax.ShapeDtypeStruct((sums, *parts[0].shape[1:]), F32),
        jax.ShapeDtypeStruct((4 * (parts[0].shape[0] - sums), *parts[0].shape[1:]), F32),
        pltpu.VMEM((width, LANES), BF16),
    ]
    spent = cost(3 * tg.size, 9 * tg.size)
    params = pltpu.CompilerParams(vmem_limit_bytes=8 * MIB)
    scale, kept, scales, *pieces = pl.pallas_call(
        lambda *refs: first_kernel(early, *refs),
        in_specs=[VMEM] * 8,
        out_specs=[VMEM] * (3 + len(early)),
        out_shape=outs + [made(k) for k, _ in early],
        compiler_params=params,
        cost_estimate=spent,
        name="scale_0",
    )(pick, *parts, tg, tu, td)
    pieces += pl.pallas_call(
        lambda *refs: rest_kernel(late, *refs),
        in_specs=[VMEM] * 5,
        out_specs=[VMEM] * len(late),
        out_shape=[made(k) for k, _ in late],
        compiler_params=params,
        cost_estimate=spent,
        name="scale_2",
    )(pick, scales, tg, tu, td)
    return scale, kept, dict(zip(early + late, pieces))


def turn_corner_kernel(*refs):
    came, outs = refs[:4], refs[4:]
    for i, out in enumerate(outs):
        for j in range(4):
            out[j] = came[j][i]


def turn_corner(came):
    out = pltpu.VMEM(came[0].shape, BF16)
    return pl.pallas_call(
        turn_corner_kernel,
        in_specs=[VMEM] * 4,
        out_specs=[VMEM] * 4,
        out_shape=[out] * 4,
        compiler_params=pltpu.CompilerParams(vmem_limit_bytes=4 * MIB),
        cost_estimate=cost(0, 16 * came[0].size),
    )(*came)


def place_kernel(picks, *refs):
    outs, done = refs[-4:-1], refs[-1]
    copies = []
    for n, ((which, i), came) in enumerate(zip(picks, refs)):
        _, _, share, _, lanes = came.shape
        for j, step in enumerate((0,) + STEPS):
            back = (-i, -step) if which % 2 == 0 else (-step, -i)
            sender = away(lax.axis_index("rows"), back)
            columns = pl.ds(pl.multiple_of(sender * lanes, lanes), lanes)
            for t, out in enumerate(outs):
                to = out.at[STARTS[which] : STARTS[which] + share, :, columns]
                copies.append(pltpu.make_async_copy(came.at[j, t], to, done.at[4 * n + j, t]))
    for copy in copies:
        copy.start()
    for copy in copies:
        copy.wait()


def side_by_side(sets, groups):
    _, _, _, rows, lanes = sets[0][0].shape
    out = pltpu.HBM((sum(SHARES), rows, 16 * lanes), BF16)
    so_far = ()
    for picks in groups:
        n = len(picks)
        so_far = pl.pallas_call(
            lambda *refs, picks=picks: place_kernel(picks, *refs),
            in_specs=[VMEM] * n + [ANY] * len(so_far),
            out_specs=[ANY] * 3,
            out_shape=[out] * 3,
            scratch_shapes=[pltpu.SemaphoreType.DMA((4 * n, 3))],
            input_output_aliases={n + t: t for t in range(len(so_far))},
            compiler_params=pltpu.CompilerParams(vmem_limit_bytes=8 * MIB),
            cost_estimate=cost(0, 4 * n * sets[0][0].size),
        )(*[sets[which][i] for which, i in picks], *so_far)
    return so_far


def order_rows_kernel(pieces, out):
    for a in range(4):
        for b in range(4):
            place = away(lax.axis_index("rows"), (-NEAR[a], -NEAR[b]))
            out[:, pl.ds(pl.multiple_of(place * LANES, LANES), LANES)] = pieces[4 * a + b].astype(BF16)


def stack_kernel(a, b, c, d, out):
    for k, part in enumerate((a, b, c, d)):
        out[k] = part[...]


def own_scales_kernel(scale, *outs):
    row = lax.axis_index("rows")
    experts, width = outs[0].shape
    group, half = lax.div(row * width, LANES), lax.rem(row * width, LANES)
    for t, out in enumerate(outs):
        x = scale[t * experts : (t + 1) * experts, group, :]
        out[...] = jnp.where(half > 0, pltpu.roll(x, LANES - width, 1), x)[:, :width]


def own_scales(scale, experts):
    out = jax.ShapeDtypeStruct((experts, 64), F32)
    return pl.pallas_call(
        own_scales_kernel,
        in_specs=[VMEM],
        out_specs=[VMEM] * 3,
        out_shape=[out] * 3,
        compiler_params=pltpu.CompilerParams(vmem_limit_bytes=4 * MIB),
        cost_estimate=cost(0, 4 * scale.size),
        name="own_scales",
    )(scale)


def order_owners_kernel(a, b, c, d, other, out):
    own = lax.axis_index("owner")
    x, core = lax.div(own, 2), lax.rem(own, 2)
    for k in range(4):
        place = lax.rem(x + 4 - k, 4) * 2
        out[pl.ds(pl.multiple_of((place + core) * 8, 8), 8), :] = (a, b, c, d)[k][...]
        out[pl.ds(pl.multiple_of((place + 1 - core) * 8, 8), 8), :] = other[k]


def placed_by(kernel, arrays, shape):
    return pl.pallas_call(
        kernel,
        in_specs=[VMEM] * len(arrays),
        out_specs=VMEM,
        out_shape=jax.ShapeDtypeStruct(shape, BF16),
        compiler_params=pltpu.CompilerParams(vmem_limit_bytes=4 * MIB),
        cost_estimate=cost(0, 1 << 18),
    )(*arrays)


def in_hbm(a):
    return pltpu.with_memory_space_constraint(a, pltpu.HBM)


def pairs(way):
    return [(i, (i // 4 + way[0]) % 4 * 4 + (i % 4 + way[1]) % 4) for i in range(16)]


ALONG_Y = [pairs((0, k)) for k in NEAR[1:]]
ALONG_Z = [pairs((k, 0)) for k in NEAR[1:]]
ALONG_X = [[(i, (i // 2 + k) % 4 * 2 + i % 2) for i in range(8)] for k in (1, 2, 3)]
OTHER_CORE = [(i, i ^ 1) for i in range(8)]


def from_all(a, axis, ways):
    came = [a]
    for way in ways:
        came.append(lax.ppermute(a, axis, way))
    return came


def body(mg, sg, mu, su, md, sd, w, gain):
    experts = mg.shape[0]
    sums = 3 * experts
    here, gate, up, td = local_sums(*[in_hbm(a) for a in (mg, sg, mu, su, md, sd, w.T, gain[None, :])])
    near = from_all(here, "rows", ALONG_Y)
    line = folded(sums, near)
    far = from_all(line, "rows", ALONG_Z)
    tg = turned(gate)
    tu = turned(up)
    scale, pieces, send = scaled(picker(sums), far, tg, tu, td)
    ways = {k: (pairs((0, k)), pairs((k, 0))) for k in STEPS}
    half = [[send[k, 0]] for k in range(SETS)]
    for k, step in sent_in_order():
        half[k].append(lax.ppermute(send[k, step], "rows", ways[step][k % 2]))
    came = []
    for k in range(SETS):
        parts = turn_corner(half[k])
        whole = [parts[0]] * 4
        for step in STEPS:
            whole[step] = lax.ppermute(parts[step], "rows", ways[step][1 - k % 2])
        came.append(whole)
    columns = placed_by(order_rows_kernel, (pieces,), (8, 16 * LANES))
    columns = from_all(columns, "owner", ALONG_X)
    other = lax.ppermute(placed_by(stack_kernel, columns, (4, 8, 16 * LANES)), "owner", OTHER_CORE)
    router = placed_by(order_owners_kernel, (*columns, other), (64, 16 * LANES)).T
    mine = own_scales(scale, experts)
    g, u, d = side_by_side(came, GROUPS)
    return (jnp.swapaxes(g, 1, 2), jnp.swapaxes(u, 1, 2), d, mine[0], mine[1], mine[2], router)


def sent_in_order(steps=STEPS):
    return [(k + i, step) for k in range(0, SETS, 2) for step in steps for i in (0, 1)]


def solution(mesh):
    placed = (
        P("owner", "rows", None),
        P("owner", "rows", None),
        P("owner", "rows", None),
        P("owner", "rows", None),
        P("owner", None, "rows"),
        P("owner", None, "rows"),
        P("rows", "owner"),
        P("rows"),
    )
    return jax.shard_map(
        body,
        mesh=mesh,
        in_specs=placed,
        out_specs=(
            P("owner", None, "rows"),
            P("owner", None, "rows"),
            P("owner", "rows", None),
            P("owner", "rows"),
            P("owner", "rows"),
            P("owner", "rows"),
            P(),
        ),
        check_vma=False,
    )
```

```python
import jax
import jax.numpy as jnp
import numpy as np
from jax import lax
from jax.experimental import pallas as pl
from jax.experimental.pallas import tpu as pltpu
from jax.sharding import PartitionSpec as P

F32, BF16 = jnp.float32, jnp.bfloat16
LANES = 128
MIB = 1 << 20


SHARES = (3, 3, 1, 1)
STARTS = (0, 3, 6, 7)
SETS = len(SHARES)
STEPS = (2, 1, 3)
NEAR = (0, 2, 1, 3)
GROUPS = (
    tuple((k, 0) for k in range(SETS)),
    ((0, 1), (1, 1), (0, 3), (1, 3)),
    ((0, 2), (1, 2), (2, 1), (3, 1), (2, 3), (3, 3)),
    ((2, 2), (3, 2)),
)


def away(row, way):
    z, y = lax.div(row, 4) + (way[0] + 4), lax.rem(row, 4) + (way[1] + 4)
    return lax.rem(z, 4) * 4 + lax.rem(y, 4)


def cost(flops, moved):
    return pl.CostEstimate(flops=flops, bytes_accessed=moved, transcendentals=0)


VMEM = pl.BlockSpec(memory_space=pltpu.VMEM)
ANY = pl.BlockSpec(memory_space=pl.ANY)


def sums_kernel(*refs):
    sources, out, merged, held = refs[:8], refs[8], refs[9:12], refs[12:20]
    columns, arrived = refs[20], refs[21]
    experts = sources[0].shape[0]
    groups = sources[4].shape[1] // LANES
    small = [
        pltpu.make_async_copy(sources[i], held[i], arrived.at[6, i - 6]) for i in (6, 7)
    ]
    for copy in small:
        copy.start()

    def fetch(i, e):
        return pltpu.make_async_copy(sources[i].at[e], held[i].at[e], arrived.at[i, e])

    for e in range(experts):
        for i in range(6):
            fetch(i, e).start()
    columns[...] = jnp.zeros_like(columns)
    for copy in small:
        copy.wait()
    out[3 * experts] = (held[6][...] * held[7][...]).astype(BF16).astype(F32)
    lane = lax.broadcasted_iota(jnp.int32, columns.shape, 1)

    def expert(e, carry):
        for t in range(2):
            fetch(2 * t, e).wait()
            fetch(2 * t + 1, e).wait()
            m, s = held[2 * t], held[2 * t + 1]
            for g in range(groups):
                part = slice(g * LANES, (g + 1) * LANES)
                x = m[e, :, part] + s[e, :, part].astype(F32)
                merged[t][e, :, part] = x
                out[t * experts + e, g : g + 1, :] = jnp.sum(x * x, axis=0, keepdims=True)
        fetch(4, e).wait()
        fetch(5, e).wait()
        so_far = columns[...]
        for g in range(groups):
            part = slice(g * LANES, (g + 1) * LANES)
            x = held[4][e, part] + held[5][e, part].astype(F32)
            merged[2][e, part] = x
            total = jnp.sum(x * x, axis=1, keepdims=True)
            so_far = jnp.where(lane == e * groups + g, total, so_far)
        columns[...] = so_far
        return carry

    lax.fori_loop(0, experts, expert, 0)
    rows = columns[...].T
    for e in range(experts):
        out[2 * experts + e] = rows[e * groups : (e + 1) * groups]


def local_sums(mg, sg, mu, su, md, sd, w, gain):
    experts, _, width = mg.shape
    arrays = (mg, sg, mu, su, md, sd, w, gain)
    return pl.pallas_call(
        sums_kernel,
        in_specs=[ANY] * 8,
        out_specs=[VMEM] * 4,
        out_shape=[jax.ShapeDtypeStruct((3 * experts + 1, width // LANES, LANES), F32)]
        + [pltpu.VMEM(a.shape, F32) for a in (mg, mu, md)],
        scratch_shapes=[pltpu.VMEM(a.shape, a.dtype) for a in arrays]
        + [pltpu.VMEM((LANES, LANES), F32), pltpu.SemaphoreType.DMA((7, experts))],
        compiler_params=pltpu.CompilerParams(vmem_limit_bytes=20 * MIB),
        cost_estimate=cost(9 * mg.size, 18 * mg.size),
        name="sums",
    )(*arrays)


def turn_kernel(m, out):
    for g in range(m.shape[2] // LANES):
        out[0, g * LANES : (g + 1) * LANES, :] = m[0, :, g * LANES : (g + 1) * LANES].T


def turned(m):
    experts, rows, width = m.shape
    return pl.pallas_call(
        turn_kernel,
        grid=(experts,),
        in_specs=[pl.BlockSpec((1, rows, width), lambda e: (e, 0, 0))],
        out_specs=pl.BlockSpec((1, width, rows), lambda e: (e, 0, 0)),
        out_shape=jax.ShapeDtypeStruct((experts, width, rows), F32),
        compiler_params=pltpu.CompilerParams(vmem_limit_bytes=8 * MIB),
        cost_estimate=cost(8 * m.size, 8 * m.size),
    )(m)


def fold_kernel(sums, a, b, c, d, out):
    out[:sums] = (a[:sums] + b[:sums]) + (c[:sums] + d[:sums])
    pieces = a.shape[0] - sums
    for k, part in enumerate((a, b, c, d)):
        out[sums + k * pieces : sums + (k + 1) * pieces] = part[sums:]


def folded(sums, parts):
    pieces = parts[0].shape[0] - sums
    out = jax.ShapeDtypeStruct((sums + 4 * pieces, *parts[0].shape[1:]), F32)
    return pl.pallas_call(
        lambda *refs: fold_kernel(sums, *refs),
        out_shape=out,
        compiler_params=pltpu.CompilerParams(vmem_limit_bytes=4 * MIB),
        cost_estimate=cost(out.size, 24 * out.size),
    )(*parts)


def in_three(x):
    high = x.astype(BF16).astype(F32)
    middle = (x - high).astype(BF16).astype(F32)
    return [high, middle, (x - high - middle).astype(BF16).astype(F32)]


def picker(combos):
    c = np.arange(LANES)[:, None]
    n = np.arange(combos * LANES)[None, :]
    return jnp.asarray((c % combos == n // LANES) & (c < 3 * combos), BF16)


def divide(picks, pick, scales, sources, outs):
    experts, _, lanes = sources[0].shape
    for (which, step), out in zip(picks, outs):
        _, _, share, width, _ = out.shape
        for i in range(4):
            way = (i, step) if which % 2 == 0 else (step, i)
            to = away(lax.axis_index("rows"), way)
            rows = pl.ds(pl.multiple_of(to * width, width), width)
            for t, source in enumerate(sources):
                first = (t * experts + STARTS[which]) * lanes
                combos = slice(first, first + share * lanes)
                scale = jnp.dot(scales[rows, :], pick[:, combos], preferred_element_type=F32)
                for e in range(share):
                    part = slice(e * lanes, (e + 1) * lanes)
                    x = source[STARTS[which] + e, rows, :]
                    out[i, t, e] = (x / scale[:, part]).astype(BF16)


def first_kernel(picks, pick, a, b, c, d, tg, tu, td, scale, kept, scales, *outs):
    sums, groups, _ = scale.shape
    root = jnp.sqrt((a[:sums] + b[:sums]) + (c[:sums] + d[:sums]))
    scale[...] = root
    pieces = a.shape[0] - sums
    for k, part in enumerate((a, b, c, d)):
        kept[k * pieces : (k + 1) * pieces] = part[sums:]
    rest = jnp.zeros((LANES - 3 * sums, LANES), F32)
    for g in range(groups):
        block = jnp.concatenate(in_three(root[:, g, :]) + [rest], axis=0)
        scales[g * LANES : (g + 1) * LANES] = block.T.astype(BF16)
    divide(picks, pick, scales, (tg, tu, td), outs)


def rest_kernel(picks, pick, scales, tg, tu, td, *outs):
    divide(picks, pick, scales, (tg, tu, td), outs)


def scaled(pick, parts, tg, tu, td):
    experts, width, rows = tg.shape
    sums = 3 * experts
    made = lambda k: pltpu.VMEM((4, 3, SHARES[k], width // 16, rows), BF16)
    early = [(k, STEPS[0]) for k in (0, 1)]
    late = [(k, step) for k in range(SETS) for step in STEPS + (0,) if (k, step) not in early]
    outs = [
        jax.ShapeDtypeStruct((sums, *parts[0].shape[1:]), F32),
        jax.ShapeDtypeStruct((4 * (parts[0].shape[0] - sums), *parts[0].shape[1:]), F32),
        pltpu.VMEM((width, LANES), BF16),
    ]
    spent = cost(3 * tg.size, 9 * tg.size)
    params = pltpu.CompilerParams(vmem_limit_bytes=8 * MIB)
    scale, kept, scales, *pieces = pl.pallas_call(
        lambda *refs: first_kernel(early, *refs),
        in_specs=[VMEM] * 8,
        out_specs=[VMEM] * (3 + len(early)),
        out_shape=outs + [made(k) for k, _ in early],
        compiler_params=params,
        cost_estimate=spent,
        name="scale_0",
    )(pick, *parts, tg, tu, td)
    pieces += pl.pallas_call(
        lambda *refs: rest_kernel(late, *refs),
        in_specs=[VMEM] * 5,
        out_specs=[VMEM] * len(late),
        out_shape=[made(k) for k, _ in late],
        compiler_params=params,
        cost_estimate=spent,
        name="scale_2",
    )(pick, scales, tg, tu, td)
    return scale, kept, dict(zip(early + late, pieces))


def turn_corner_kernel(*refs):
    came, outs = refs[:4], refs[4:]
    for i, out in enumerate(outs):
        for j in range(4):
            out[j] = came[j][i]


def turn_corner(came):
    out = pltpu.VMEM(came[0].shape, BF16)
    return pl.pallas_call(
        turn_corner_kernel,
        in_specs=[VMEM] * 4,
        out_specs=[VMEM] * 4,
        out_shape=[out] * 4,
        compiler_params=pltpu.CompilerParams(vmem_limit_bytes=4 * MIB),
        cost_estimate=cost(0, 16 * came[0].size),
    )(*came)


def place_kernel(picks, *refs):
    outs, done = refs[-4:-1], refs[-1]
    copies = []
    for n, ((which, i), came) in enumerate(zip(picks, refs)):
        _, _, share, _, lanes = came.shape
        for j, step in enumerate((0,) + STEPS):
            back = (-i, -step) if which % 2 == 0 else (-step, -i)
            sender = away(lax.axis_index("rows"), back)
            columns = pl.ds(pl.multiple_of(sender * lanes, lanes), lanes)
            for t, out in enumerate(outs):
                to = out.at[STARTS[which] : STARTS[which] + share, :, columns]
                copies.append(pltpu.make_async_copy(came.at[j, t], to, done.at[4 * n + j, t]))
    for copy in copies:
        copy.start()
    for copy in copies:
        copy.wait()


def side_by_side(sets, groups):
    _, _, _, rows, lanes = sets[0][0].shape
    out = pltpu.HBM((sum(SHARES), rows, 16 * lanes), BF16)
    so_far = ()
    for picks in groups:
        n = len(picks)
        so_far = pl.pallas_call(
            lambda *refs, picks=picks: place_kernel(picks, *refs),
            in_specs=[VMEM] * n + [ANY] * len(so_far),
            out_specs=[ANY] * 3,
            out_shape=[out] * 3,
            scratch_shapes=[pltpu.SemaphoreType.DMA((4 * n, 3))],
            input_output_aliases={n + t: t for t in range(len(so_far))},
            compiler_params=pltpu.CompilerParams(vmem_limit_bytes=8 * MIB),
            cost_estimate=cost(0, 4 * n * sets[0][0].size),
        )(*[sets[which][i] for which, i in picks], *so_far)
    return so_far


def order_rows_kernel(pieces, out):
    for a in range(4):
        for b in range(4):
            place = away(lax.axis_index("rows"), (-NEAR[a], -NEAR[b]))
            out[:, pl.ds(pl.multiple_of(place * LANES, LANES), LANES)] = pieces[4 * a + b].astype(BF16)


def stack_kernel(a, b, c, d, out):
    for k, part in enumerate((a, b, c, d)):
        out[k] = part[...]


def own_scales_kernel(scale, *outs):
    row = lax.axis_index("rows")
    experts, width = outs[0].shape
    group, half = lax.div(row * width, LANES), lax.rem(row * width, LANES)
    for t, out in enumerate(outs):
        x = scale[t * experts : (t + 1) * experts, group, :]
        out[...] = jnp.where(half > 0, pltpu.roll(x, LANES - width, 1), x)[:, :width]


def own_scales(scale, experts):
    out = jax.ShapeDtypeStruct((experts, 64), F32)
    return pl.pallas_call(
        own_scales_kernel,
        in_specs=[VMEM],
        out_specs=[VMEM] * 3,
        out_shape=[out] * 3,
        compiler_params=pltpu.CompilerParams(vmem_limit_bytes=4 * MIB),
        cost_estimate=cost(0, 4 * scale.size),
        name="own_scales",
    )(scale)


def order_owners_kernel(a, b, c, d, other, out):
    own = lax.axis_index("owner")
    x, core = lax.div(own, 2), lax.rem(own, 2)
    for k in range(4):
        place = lax.rem(x + 4 - k, 4) * 2
        out[pl.ds(pl.multiple_of((place + core) * 8, 8), 8), :] = (a, b, c, d)[k][...]
        out[pl.ds(pl.multiple_of((place + 1 - core) * 8, 8), 8), :] = other[k]


def placed_by(kernel, arrays, shape):
    return pl.pallas_call(
        kernel,
        in_specs=[VMEM] * len(arrays),
        out_specs=VMEM,
        out_shape=jax.ShapeDtypeStruct(shape, BF16),
        compiler_params=pltpu.CompilerParams(vmem_limit_bytes=4 * MIB),
        cost_estimate=cost(0, 1 << 18),
    )(*arrays)


def in_hbm(a):
    return pltpu.with_memory_space_constraint(a, pltpu.HBM)


def pairs(way):
    return [(i, (i // 4 + way[0]) % 4 * 4 + (i % 4 + way[1]) % 4) for i in range(16)]


ALONG_Y = [pairs((0, k)) for k in NEAR[1:]]
ALONG_Z = [pairs((k, 0)) for k in NEAR[1:]]
ALONG_X = [[(i, (i // 2 + k) % 4 * 2 + i % 2) for i in range(8)] for k in (1, 2, 3)]
OTHER_CORE = [(i, i ^ 1) for i in range(8)]


def from_all(a, axis, ways):
    came = [a]
    for way in ways:
        came.append(lax.ppermute(a, axis, way))
    return came


def body(mg, sg, mu, su, md, sd, w, gain):
    experts = mg.shape[0]
    sums = 3 * experts
    here, gate, up, td = local_sums(*[in_hbm(a) for a in (mg, sg, mu, su, md, sd, w.T, gain[None, :])])
    near = from_all(here, "rows", ALONG_Y)
    line = folded(sums, near)
    far = from_all(line, "rows", ALONG_Z)
    tg = turned(gate)
    tu = turned(up)
    scale, pieces, send = scaled(picker(sums), far, tg, tu, td)
    ways = {k: (pairs((0, k)), pairs((k, 0))) for k in STEPS}
    half = [[send[k, 0]] for k in range(SETS)]
    for k, step in sent_in_order():
        half[k].append(lax.ppermute(send[k, step], "rows", ways[step][k % 2]))
    came = []
    for k in range(SETS):
        parts = turn_corner(half[k])
        whole = [parts[0]] * 4
        for step in STEPS:
            whole[step] = lax.ppermute(parts[step], "rows", ways[step][1 - k % 2])
        came.append(whole)
    columns = placed_by(order_rows_kernel, (pieces,), (8, 16 * LANES))
    columns = from_all(columns, "owner", ALONG_X)
    other = lax.ppermute(placed_by(stack_kernel, columns, (4, 8, 16 * LANES)), "owner", OTHER_CORE)
    router = placed_by(order_owners_kernel, (*columns, other), (64, 16 * LANES)).T
    mine = own_scales(scale, experts)
    g, u, d = side_by_side(came, GROUPS)
    return (jnp.swapaxes(g, 1, 2), jnp.swapaxes(u, 1, 2), d, mine[0], mine[1], mine[2], router)


def sent_in_order(steps=STEPS):
    return [(k + i, step) for k in range(0, SETS, 2) for step in steps for i in (0, 1)]


def solution(mesh):
    placed = (
        P("owner", "rows", None),
        P("owner", "rows", None),
        P("owner", "rows", None),
        P("owner", "rows", None),
        P("owner", None, "rows"),
        P("owner", None, "rows"),
        P("rows", "owner"),
        P("rows"),
    )
    return jax.shard_map(
        body,
        mesh=mesh,
        in_specs=placed,
        out_specs=(
            P("owner", None, "rows"),
            P("owner", None, "rows"),
            P("owner", "rows", None),
            P("owner", "rows"),
            P("owner", "rows"),
            P("owner", "rows"),
            P(),
        ),
        check_vma=False,
    )
```
